32 devices in a mesh: occ: 16 (over z, y, x), aux: 2 (over core).
Axes of the slice: x: 2, y: 2, z: 4, core: 2. Of those that a mesh axis runs over, the one named last changes fastest.
Arguments:
- factors: bfloat16 [7680, 16, 768], P('aux', 'occ'), may hold values from -0.71875 to 0.71875
- occ_energy: float32 [16], replicated, may hold values from -3 to -0.3
- virt_energy: float32 [768], replicated, may hold values from 0.3 to 3
Outputs:
- gradient: float32 [7680, 16, 768], P('aux', 'occ')
The draws below stay inside these ranges and needn't reach their ends.
All inputs are finite; a program needn't handle non-finite values.
Results may differ from the reference program's by a relative error of at most 0.0027.
Values may be sent and summed in bfloat16 or wider, within the bound.
No kernel may reach another device: no remote copies, remote signals or barrier semaphores. Data moves between devices by JAX's collectives and lax.ppermute only.
A program may use at most 64 MiB of HBM per device.

```python
import math
import jax
import jax.numpy as jnp
from jax import lax

V = 768
NAUX = 7680
OCC_DEV = 1
O = 16
N_OCC = 16


def steps_of(own_key, shape, shards, low, high):
    def one(dim, parts):
        heights = jax.random.uniform(jax.random.fold_in(jax.random.fold_in(own_key, 6), dim), (parts,), jnp.float32, low / len(shards), high / len(shards))
        return jnp.repeat(jnp.exp(heights), shape[dim] // parts).reshape((-1,) + (1,) * (len(shape) - dim - 1))

    loudness = one(*shards[0])
    for cut in shards[1:]:
        loudness = loudness * one(*cut)
    return loudness


def bell_draw(key, dims, deviation, bound, pieces=(), held_as=jnp.bfloat16):
    entries = deviation * jax.random.normal(key, dims, jnp.float32)
    if pieces:
        entries = entries * steps_of(key, dims, pieces, -0.22, 0.18)
    return jnp.clip(entries, -bound, bound).astype(held_as)


def setup_inputs(seed: int = 0) -> dict:
    key_of = jax.random.split(jax.random.key(seed), 4)
    factors = bell_draw(key_of[0], (NAUX, O, V), 0.12, 0.71875, ((0, 2), (1, 16)))
    occ_energy = jnp.clip(jax.random.uniform(key_of[1], (O,), jnp.float32, -3.0, -0.3), -3.0, -0.3)
    virt_energy = jnp.clip(jnp.exp(jax.random.uniform(key_of[2], (V,), jnp.float32, math.log(0.3), math.log(3.0))), 0.3, 3.0)
    return dict(factors=factors, occ_energy=occ_energy, virt_energy=virt_energy)


def pair_tilde(left, right, e_left, e_right, virt_energy):
    whole = jnp.dot(left.astype(jnp.float32).T, right.astype(jnp.float32))
    width = virt_energy.shape[0]
    count = e_left.shape[0]
    denom = (virt_energy[None, :, None, None] + virt_energy[None, None, None, :]
             - e_left[:, None, None, None] - e_right[None, None, :, None])
    amplitude = whole.reshape(count, width, count, width) / denom
    tilde = (2.0 * amplitude - amplitude.transpose(0, 3, 2, 1)).astype(jnp.bfloat16)
    return tilde.reshape(count * width, count * width)


def reference(factors, occ_energy, virt_energy):
    offset = N_OCC // 4
    flat = factors.reshape(NAUX, N_OCC, OCC_DEV * V)
    start = jnp.zeros((N_OCC, NAUX, OCC_DEV * V), jnp.float32)

    def step(carry, block):
        partner_block = (block + offset) % N_OCC
        left = lax.dynamic_index_in_dim(flat, block, 1, keepdims=False)
        right = lax.dynamic_index_in_dim(flat, partner_block, 1, keepdims=False)
        e_left = lax.dynamic_slice_in_dim(occ_energy, (block * OCC_DEV).astype(jnp.int32), OCC_DEV)
        e_right = lax.dynamic_slice_in_dim(occ_energy, (partner_block * OCC_DEV).astype(jnp.int32), OCC_DEV)
        tilde = pair_tilde(left, right, e_left, e_right, virt_energy).astype(jnp.float32)
        own = jnp.dot(right.astype(jnp.float32), tilde.T)
        partner = jnp.dot(left.astype(jnp.float32), tilde)
        carry = carry.at[block].add(own)
        carry = carry.at[partner_block].add(partner)
        return carry, None

    total, _ = lax.scan(step, start, jnp.arange(N_OCC, dtype=jnp.int32))
    return total.transpose(1, 0, 2).reshape(NAUX, N_OCC * OCC_DEV, V)
```

```python
import functools
import math

import jax
import jax.numpy as jnp
from jax import lax
from jax.experimental import pallas as pl
from jax.experimental.pallas import tpu as pltpu
from jax.sharding import PartitionSpec as P


LANES = 128
F32 = jnp.float32
BF16 = jnp.bfloat16
ROWS_IN = (((0,), (0,)), ((), ()))


def largest_block(rows, most):
    return max(size for size in range(16, most + 1, 16) if rows % size == 0)


def swapped(value):
    return lax.ppermute(value, "aux", [(0, 1), (1, 0)])


def aux_terms(value):
    if lax.axis_size("aux") == 2:
        return [value, swapped(value)]
    return [lax.psum(value, "aux")]


def gram(left, right):
    return lax.dot_general(left, right, ROWS_IN, preferred_element_type=F32)


def on_chip(value):
    return pltpu.with_memory_space_constraint(value, pltpu.VMEM)


def fill_tilde(tilde, amp, sums, pairs, across, e_left, e_right):
    width = tilde.shape[0]
    for at in range(0, width, LANES):
        here = pl.ds(at, LANES)
        whole = sums[0][here, :]
        for other in sums[1:]:
            whole = whole + other[here, :]
        for left, right in pairs:
            whole = whole + gram(left[:, at : at + LANES], right[...])
        down = jnp.transpose(jnp.broadcast_to(across[:, at : at + LANES], (LANES, LANES)))
        amp[here, :] = whole / (down[:, :1] + across - e_left - e_right)
    for at in range(0, width, LANES):
        here = pl.ds(at, LANES)
        tilde[here, :] = (2.0 * amp[here, :] - jnp.transpose(amp[:, at : at + LANES])).astype(BF16)


def gram_kernel(block, offset, has_start, *refs):
    start, left, right, out = refs if has_start else (None, *refs)
    out[...] = start[...] if has_start else jnp.zeros_like(out)

    @pl.loop(0, left.shape[0] // block)
    def _(step):
        rows = left[pl.ds(pl.multiple_of(step * block, block), block), :]
        others = right[pl.ds(pl.multiple_of(offset + step * block, math.gcd(offset, block)), block), :]
        out[...] += gram(rows, others)


def gram_stage(left, right, offset=0, start=None):
    width = right.shape[1]
    vmem = pl.BlockSpec(memory_space=pltpu.VMEM)
    operands = [value for value in (start, left, right) if value is not None]
    return pl.pallas_call(
        functools.partial(gram_kernel, largest_block(left.shape[0], 640), offset, start is not None),
        in_specs=[vmem] * len(operands),
        out_specs=vmem,
        out_shape=pltpu.VMEM((width, width), F32),
        compiler_params=pltpu.CompilerParams(vmem_limit_bytes=10 << 20),
        cost_estimate=pl.CostEstimate(flops=2 * left.size * width, bytes_accessed=0, transcendentals=0),
        name="gram_stage",
    )(*[on_chip(value) for value in operands])


def near_kernel(block, n_sums, energy, virt_row, *refs):
    sums, (behind, ahead, out, amp, *tildes) = refs[: 2 * n_sums], refs[2 * n_sums :]
    across = virt_row[...]
    for item, tilde in enumerate(tildes):
        terms = sums[item * n_sums : (item + 1) * n_sums]
        fill_tilde(tilde, amp, terms, [], across, energy[2 * item], energy[2 * item + 1])

    @pl.loop(0, out.shape[0] // block)
    def _(step):
        here = pl.ds(pl.multiple_of(step * block, block), block)
        first = jnp.dot(behind[here, :], tildes[0][...], preferred_element_type=F32)
        out[here, :] = first + jnp.dot(ahead[here, :], tildes[1][...], preferred_element_type=F32)


def near_stage(energy, virt_row, sums, behind, ahead, block):
    rows, width = behind.shape
    vmem = pl.BlockSpec(memory_space=pltpu.VMEM)
    operands = [virt_row, *sums, behind, ahead]
    return pl.pallas_call(
        functools.partial(near_kernel, block, len(sums) // 2),
        in_specs=[pl.BlockSpec(memory_space=pltpu.SMEM)] + [vmem] * len(operands),
        out_specs=vmem,
        out_shape=pltpu.VMEM((rows, width), F32),
        scratch_shapes=[pltpu.VMEM((width, width), F32)] + [pltpu.VMEM((width, width), BF16)] * 2,
        compiler_params=pltpu.CompilerParams(vmem_limit_bytes=16 << 20),
        cost_estimate=pl.CostEstimate(flops=4 * rows * width * width, bytes_accessed=0, transcendentals=0),
        name="near_stage",
    )(energy, *[on_chip(value) for value in operands])


def far_kernel(block, n_sums, n_pairs, heights, energy, virt_row, *refs):
    refs = list(refs)
    sums = [refs.pop(0) for _ in range(n_sums)]
    pairs = [(refs.pop(0), refs.pop(0)) for _ in range(n_pairs)]
    parts = [refs.pop(0) for _ in heights]
    base, out, amp, tilde, out_buf, out_sem = refs
    width = tilde.shape[0]
    strips = width // LANES
    fill_tilde(tilde, amp, sums, pairs, virt_row[...], energy[0], energy[1])

    jobs, first = [], 0
    for part, height in zip(parts, heights):
        for at in range(0, height, block):
            jobs.append((part, at, first + at, min(block, height - at)))
        first += height

    def copy(job):
        _, _, row, tall = jobs[job]
        rows = pl.ds(0, tall * strips)
        return pltpu.make_async_copy(
            out_buf.at[job % 2, rows, :], out.at[pl.ds(row * strips, tall * strips), :], out_sem.at[job % 2]
        )

    for job, (part, at, row, tall) in enumerate(jobs):
        term = jnp.dot(part[pl.ds(at, tall), :], tilde[...], preferred_element_type=F32)
        result = base[pl.ds(row, tall), :] + term
        if job >= 2:
            copy(job - 2).wait()
        for strip in range(strips):
            out_buf[job % 2, pl.ds(strip, tall, strips), :] = result[:, strip * LANES : (strip + 1) * LANES]
        copy(job).start()
    for job in range(max(0, len(jobs) - 2), len(jobs)):
        copy(job).wait()


def far_stage(energy, virt_row, sums, pairs, parts, base, block):
    rows, width = base.shape
    strips = width // LANES
    vmem = pl.BlockSpec(memory_space=pltpu.VMEM)
    operands = [virt_row, *sums, *[value for pair in pairs for value in pair], *parts, base]
    heights = tuple(part.shape[0] for part in parts)
    return pl.pallas_call(
        functools.partial(far_kernel, block, len(sums), len(pairs), heights),
        in_specs=[pl.BlockSpec(memory_space=pltpu.SMEM)] + [vmem] * len(operands),
        out_specs=pl.BlockSpec(memory_space=pl.ANY),
        out_shape=jax.ShapeDtypeStruct((rows * strips, LANES), F32),
        scratch_shapes=[
            pltpu.VMEM((width, width), F32),
            pltpu.VMEM((width, width), BF16),
            pltpu.VMEM((2, block * strips, LANES), F32),
            pltpu.SemaphoreType.DMA((2,)),
        ],
        compiler_params=pltpu.CompilerParams(vmem_limit_bytes=20 << 20),
        cost_estimate=pl.CostEstimate(
            flops=2 * rows * width * width, bytes_accessed=4 * rows * width, transcendentals=0
        ),
        name="far_stage",
    )(energy, *[on_chip(value) for value in operands])


def plain(factors, occ_energy, virt_energy):
    rows, count, width = factors.shape
    n_blocks = lax.axis_size("occ")
    offset = n_blocks // 4
    index = lax.axis_index("occ")
    total = jnp.zeros((rows, count, width), F32)
    own_e = lax.dynamic_slice_in_dim(occ_energy, index * count, count)
    for steps, first in ((-offset, True), (offset, False)):
        ring = [(source, (source + steps) % n_blocks) for source in range(n_blocks)]
        other = lax.ppermute(factors, "occ", ring)
        other_e = lax.dynamic_slice_in_dim(occ_energy, (index - steps) % n_blocks * count, count)
        whole = sum(aux_terms(jnp.einsum("pja,pib->jaib", other, factors, preferred_element_type=F32)))
        e_left, e_right = (own_e[None, None, :, None], other_e[:, None, None, None])
        if not first:
            e_left, e_right = e_right, e_left
        amplitude = whole / (virt_energy[None, :, None, None] + virt_energy - e_left - e_right)
        tilde = (2.0 * amplitude - amplitude.transpose(0, 3, 2, 1)).astype(BF16)
        total = total + jnp.einsum("pja,jaib->pib", other, tilde, preferred_element_type=F32)
    return total


def far_cuts(rows, unit):
    steps = rows // unit
    if lax.axis_size("aux") != 2 or steps < 4:
        return [0, rows], 0
    return [0, (steps * 2 // 5) * unit, (steps * 4 // 5) * unit, (steps - 2) * unit, (steps - 1) * unit, rows], 2


def local(factors, occ_energy, virt_energy):
    rows, count, width = factors.shape
    n_blocks = lax.axis_size("occ")
    if count != 1 or width % LANES or rows % 16:
        return plain(factors, occ_energy, virt_energy)
    offset = n_blocks // 4
    index = lax.axis_index("occ")
    cuts, n_late = far_cuts(rows, largest_block(rows, 256))

    up = [(s, s + offset) for s in range(n_blocks - offset)]
    down = [(s + offset, s) for s in range(n_blocks - offset)]
    ends = [(s, s + n_blocks - offset) for s in range(offset)]
    ends = ends + [(t, s) for s, t in ends]

    own = factors.reshape(rows, width)
    pieces = [own[a:b] for a, b in zip(cuts[:-1], cuts[1:])]
    behind = lax.ppermute(own, "occ", up)
    ahead = lax.ppermute(own, "occ", down)
    *pieces, behind, ahead = lax.optimization_barrier((*pieces, behind, ahead))
    far = []
    for piece in pieces:
        far.append(lax.ppermute(piece, "occ", ends))

    e_own = occ_energy[index]
    e_ahead = occ_energy[(index + offset) % n_blocks]
    e_behind = occ_energy[(index - offset) % n_blocks]
    virt_row = virt_energy.reshape(1, width)

    last = index >= n_blocks - offset
    energy = jnp.stack([e_behind, e_own, e_own, e_ahead])
    far_energy = jnp.stack([jnp.where(last, e_own, e_behind), jnp.where(last, e_ahead, e_own)])
    others = [swapped(piece) for piece in pieces[len(pieces) - n_late :]]
    energy, far_energy, *others = lax.optimization_barrier((energy, far_energy, *others))
    grams = [gram_stage(behind, own), gram_stage(ahead, own)]
    sums = aux_terms(grams[0]) + aux_terms(grams[1])
    base = near_stage(energy, virt_row, sums, behind, ahead, largest_block(rows, 480))

    far[0], base = lax.optimization_barrier((far[0], base))
    early = None
    for part, at in list(zip(far, cuts))[: len(far) - n_late]:
        if early is not None:
            part, early = lax.optimization_barrier((part, early))
        early = gram_stage(part, own, at, early)
    sums = aux_terms(early)
    pairs = []
    for part, piece, other in zip(far[len(far) - n_late :], pieces[len(far) - n_late :], others):
        pairs += [(part, piece), (swapped(part), other)]
    out = far_stage(far_energy, virt_row, sums, pairs, far, base, largest_block(rows, 960))
    return out.reshape(rows, count, width)


def solution(mesh):
    in_specs = (P("aux", "occ", None), P(), P())
    out_specs = P("aux", "occ", None)

    return jax.shard_map(local, mesh=mesh, in_specs=in_specs, out_specs=out_specs, check_vma=False)
```

```python
import functools
import math

import jax
import jax.numpy as jnp
from jax import lax
from jax.experimental import pallas as pl
from jax.experimental.pallas import tpu as pltpu
from jax.sharding import PartitionSpec as P


LANES = 128
NEAR_SHARES = (24, 204, 12)
FAR_SHARES = (96, 96, 21, 15, 12)
NEAR_VMEM = 18 << 20
F32 = jnp.float32
BF16 = jnp.bfloat16
ROWS_IN = (((0,), (0,)), ((), ()))


def largest_block(rows, most):
    return max(size for size in range(16, most + 1, 16) if rows % size == 0)


def swapped(value):
    return lax.ppermute(value, "aux", [(0, 1), (1, 0)])


def aux_terms(value):
    if lax.axis_size("aux") == 2:
        return [value, swapped(value)]
    return [lax.psum(value, "aux")]


def gram(left, right):
    return lax.dot_general(left, right, ROWS_IN, preferred_element_type=F32)


def on_chip(value):
    return pltpu.with_memory_space_constraint(value, pltpu.VMEM)


def fill_tilde(tilde, amp, sums, pairs, across, e_left, e_right):
    width = tilde.shape[0]
    for left, right in pairs:
        amp[...] = gram(left[...], right[...])
        sums = [*sums, amp]
    for at in range(0, width, LANES):
        here = pl.ds(at, LANES)
        whole = sums[0][here, :]
        for other in sums[1:]:
            whole = whole + other[here, :]
        down = jnp.transpose(jnp.broadcast_to(across[:, at : at + LANES], (LANES, LANES)))
        amp[here, :] = whole / (down[:, :1] + across - e_left - e_right)
    for at in range(0, width, LANES):
        here = pl.ds(at, LANES)
        tilde[here, :] = (2.0 * amp[here, :] - jnp.transpose(amp[:, at : at + LANES])).astype(BF16)


def gram_kernel(block, offset, has_start, *refs):
    start, left, right, out = refs if has_start else (None, *refs)
    out[...] = start[...] if has_start else jnp.zeros_like(out)

    @pl.loop(0, left.shape[0] // block)
    def _(step):
        rows = left[pl.ds(pl.multiple_of(step * block, block), block), :]
        others = right[pl.ds(pl.multiple_of(offset + step * block, math.gcd(offset, block)), block), :]
        out[...] += gram(rows, others)


def gram_stage(left, right, offset=0, start=None):
    width = right.shape[1]
    vmem = pl.BlockSpec(memory_space=pltpu.VMEM)
    operands = [value for value in (start, left, right) if value is not None]
    return pl.pallas_call(
        functools.partial(gram_kernel, largest_block(left.shape[0], 640), offset, start is not None),
        in_specs=[vmem] * len(operands),
        out_specs=vmem,
        out_shape=pltpu.VMEM((width, width), F32),
        compiler_params=pltpu.CompilerParams(vmem_limit_bytes=10 << 20),
        cost_estimate=pl.CostEstimate(flops=2 * left.size * width, bytes_accessed=0, transcendentals=0),
        name="gram_stage",
    )(*[on_chip(value) for value in operands])


def near_kernel(n_sums, heights, energy, virt_row, *refs):
    sums, refs = refs[: 2 * n_sums], refs[2 * n_sums :]
    behind, ahead = refs[: len(heights)], refs[len(heights) : 2 * len(heights)]
    out, amp, *tildes = refs[2 * len(heights) :]
    across = virt_row[...]
    for item, tilde in enumerate(tildes):
        terms = sums[item * n_sums : (item + 1) * n_sums]
        fill_tilde(tilde, amp, terms, [], across, energy[2 * item], energy[2 * item + 1])

    first = 0
    for height, left, right in zip(heights, behind, ahead):
        block = largest_block(height, 640)

        @pl.loop(0, height // block)
        def _(step, first=first, block=block, left=left, right=right):
            here = pl.ds(pl.multiple_of(step * block, block), block)
            there = pl.ds(pl.multiple_of(first + step * block, math.gcd(first, block)), block)
            term = jnp.dot(left[here, :], tildes[0][...], preferred_element_type=F32)
            out[there, :] = term + jnp.dot(right[here, :], tildes[1][...], preferred_element_type=F32)

        first += height


def near_stage(energy, virt_row, sums, behind, ahead):
    heights = tuple(part.shape[0] for part in behind)
    rows, width = sum(heights), behind[0].shape[1]
    vmem = pl.BlockSpec(memory_space=pltpu.VMEM)
    operands = [virt_row, *sums, *behind, *ahead]
    return pl.pallas_call(
        functools.partial(near_kernel, len(sums) // 2, heights),
        in_specs=[pl.BlockSpec(memory_space=pltpu.SMEM)] + [vmem] * len(operands),
        out_specs=vmem,
        out_shape=pltpu.VMEM((rows, width), F32),
        scratch_shapes=[pltpu.VMEM((width, width), F32)] + [pltpu.VMEM((width, width), BF16)] * 2,
        compiler_params=pltpu.CompilerParams(vmem_limit_bytes=NEAR_VMEM),
        cost_estimate=pl.CostEstimate(flops=4 * rows * width * width, bytes_accessed=0, transcendentals=0),
        name="near_stage",
    )(energy, *[on_chip(value) for value in operands])


def far_kernel(block, n_sums, n_pairs, heights, energy, virt_row, *refs):
    refs = list(refs)
    sums = [refs.pop(0) for _ in range(n_sums)]
    pairs = [(refs.pop(0), refs.pop(0)) for _ in range(n_pairs)]
    parts = [refs.pop(0) for _ in heights]
    base, out, amp, tilde, out_buf, out_sem = refs
    width = tilde.shape[0]
    strips = width // LANES
    fill_tilde(tilde, amp, sums, pairs, virt_row[...], energy[0], energy[1])

    jobs, first = [], 0
    for part, height in zip(parts, heights):
        for at in range(0, height, block):
            jobs.append((part, at, first + at, min(block, height - at)))
        first += height

    def copy(job):
        _, _, row, tall = jobs[job]
        rows = pl.ds(0, tall * strips)
        return pltpu.make_async_copy(
            out_buf.at[job % 2, rows, :], out.at[pl.ds(row * strips, tall * strips), :], out_sem.at[job % 2]
        )

    for job, (part, at, row, tall) in enumerate(jobs):
        term = jnp.dot(part[pl.ds(at, tall), :], tilde[...], preferred_element_type=F32)
        result = base[pl.ds(row, tall), :] + term
        if job >= 2:
            copy(job - 2).wait()
        for strip in range(strips):
            out_buf[job % 2, pl.ds(strip, tall, strips), :] = result[:, strip * LANES : (strip + 1) * LANES]
        copy(job).start()
    for job in range(max(0, len(jobs) - 2), len(jobs)):
        copy(job).wait()


def far_stage(energy, virt_row, sums, pairs, parts, base, block):
    rows, width = base.shape
    strips = width // LANES
    vmem = pl.BlockSpec(memory_space=pltpu.VMEM)
    operands = [virt_row, *sums, *[value for pair in pairs for value in pair], *parts, base]
    heights = tuple(part.shape[0] for part in parts)
    return pl.pallas_call(
        functools.partial(far_kernel, block, len(sums), len(pairs), heights),
        in_specs=[pl.BlockSpec(memory_space=pltpu.SMEM)] + [vmem] * len(operands),
        out_specs=pl.BlockSpec(memory_space=pl.ANY),
        out_shape=jax.ShapeDtypeStruct((rows * strips, LANES), F32),
        scratch_shapes=[
            pltpu.VMEM((width, width), F32),
            pltpu.VMEM((width, width), BF16),
            pltpu.VMEM((2, block * strips, LANES), F32),
            pltpu.SemaphoreType.DMA((2,)),
        ],
        compiler_params=pltpu.CompilerParams(vmem_limit_bytes=20 << 20),
        cost_estimate=pl.CostEstimate(
            flops=2 * rows * width * width, bytes_accessed=4 * rows * width, transcendentals=0
        ),
        name="far_stage",
    )(energy, *[on_chip(value) for value in operands])


def plain(factors, occ_energy, virt_energy):
    rows, count, width = factors.shape
    n_blocks = lax.axis_size("occ")
    offset = n_blocks // 4
    index = lax.axis_index("occ")
    total = jnp.zeros((rows, count, width), F32)
    own_e = lax.dynamic_slice_in_dim(occ_energy, index * count, count)
    for steps, first in ((-offset, True), (offset, False)):
        ring = [(source, (source + steps) % n_blocks) for source in range(n_blocks)]
        other = lax.ppermute(factors, "occ", ring)
        other_e = lax.dynamic_slice_in_dim(occ_energy, (index - steps) % n_blocks * count, count)
        whole = sum(aux_terms(jnp.einsum("pja,pib->jaib", other, factors, preferred_element_type=F32)))
        e_left, e_right = (own_e[None, None, :, None], other_e[:, None, None, None])
        if not first:
            e_left, e_right = e_right, e_left
        amplitude = whole / (virt_energy[None, :, None, None] + virt_energy - e_left - e_right)
        tilde = (2.0 * amplitude - amplitude.transpose(0, 3, 2, 1)).astype(BF16)
        total = total + jnp.einsum("pja,jaib->pib", other, tilde, preferred_element_type=F32)
    return total


def cuts_of(rows, shares):
    unit, rest = divmod(rows, sum(shares))
    if rest or unit % 16:
        return [0, rows]
    return [unit * sum(shares[:at]) for at in range(len(shares) + 1)]


def sent(pieces, ring):
    arrived = []
    for piece in pieces:
        arrived.append(lax.ppermute(piece, "occ", ring))
    return arrived


def grams_of(parts, own, cuts, start=None):
    for part, at in zip(parts, cuts):
        if start is not None:
            part, start = lax.optimization_barrier((part, start))
        start = gram_stage(part, own, at, start)
    return start


def local(factors, occ_energy, virt_energy):
    rows, count, width = factors.shape
    n_blocks = lax.axis_size("occ")
    if count != 1 or width % LANES or rows % 16:
        return plain(factors, occ_energy, virt_energy)
    offset = n_blocks // 4
    index = lax.axis_index("occ")
    near_cuts, far_cuts, n_late = [0, rows], [0, rows], 0
    if lax.axis_size("aux") == 2:
        near_cuts = cuts_of(rows, NEAR_SHARES)
        far_cuts = cuts_of(rows, FAR_SHARES)
        n_late = int(len(far_cuts) > 2)

    up = [(s, s + offset) for s in range(n_blocks - offset)]
    down = [(s + offset, s) for s in range(n_blocks - offset)]
    ends = [(s, s + n_blocks - offset) for s in range(offset)]
    ends = ends + [(t, s) for s, t in ends]

    own = factors.reshape(rows, width)
    pieces = [own[a:b] for a, b in zip(near_cuts[:-1], near_cuts[1:])]
    behind, ahead = sent(pieces, up), sent(pieces, down)

    pieces = [own[a:b] for a, b in zip(far_cuts[:-1], far_cuts[1:])]
    at = max(0, len(behind) - 2)
    pieces[0], behind[at], ahead[at] = lax.optimization_barrier((pieces[0], behind[at], ahead[at]))
    *pieces[1:], behind[-1], ahead[-1] = lax.optimization_barrier((*pieces[1:], behind[-1], ahead[-1]))
    far = sent(pieces, ends)

    e_own = occ_energy[index]
    e_ahead = occ_energy[(index + offset) % n_blocks]
    e_behind = occ_energy[(index - offset) % n_blocks]
    virt_row = virt_energy.reshape(1, width)

    last = index >= n_blocks - offset
    energy = jnp.stack([e_behind, e_own, e_own, e_ahead])
    far_energy = jnp.stack([jnp.where(last, e_own, e_behind), jnp.where(last, e_ahead, e_own)])
    others = [swapped(piece) for piece in pieces[len(pieces) - n_late :]]
    energy, far_energy, *others = lax.optimization_barrier((energy, far_energy, *others))
    grams = [grams_of(parts[:-1], own, near_cuts) for parts in (behind, ahead)]
    close = [grams_of(parts[-1:], own, near_cuts[-2:-1], start) for parts, start in zip((behind, ahead), grams)]
    grams = close
    sums = aux_terms(grams[0]) + aux_terms(grams[1])
    base = near_stage(energy, virt_row, sums, behind, ahead)

    far[0], base = lax.optimization_barrier((far[0], base))
    sums = aux_terms(grams_of(far[: len(far) - n_late], own, far_cuts))
    pairs = []
    if n_late:
        pairs = [(swapped(far[-1]), others[0])]
        sums[0] = gram_stage(far[-1], own, far_cuts[-2], sums[0])
    out = far_stage(far_energy, virt_row, sums, pairs, far, base, min(rows, 768))
    return out.reshape(rows, count, width)


def solution(mesh):
    in_specs = (P("aux", "occ", None), P(), P())
    out_specs = P("aux", "occ", None)

    return jax.shard_map(local, mesh=mesh, in_specs=in_specs, out_specs=out_specs, check_vma=False)
```

```python
import functools
import math

import jax
import jax.numpy as jnp
from jax import lax
from jax.experimental import pallas as pl
from jax.experimental.pallas import tpu as pltpu
from jax.sharding import PartitionSpec as P


LANES = 128
NEAR_SHARES = (24, 210, 6)
FAR_SHARES = (96, 96, 21, 15, 12)
NEAR_VMEM = 18 << 20
F32 = jnp.float32
BF16 = jnp.bfloat16
ROWS_IN = (((0,), (0,)), ((), ()))


def largest_block(rows, most):
    return max(size for size in range(16, most + 1, 16) if rows % size == 0)


def swapped(value):
    return lax.ppermute(value, "aux", [(0, 1), (1, 0)])


def aux_terms(value):
    if lax.axis_size("aux") == 2:
        return [value, swapped(value)]
    return [lax.psum(value, "aux")]


def gram(left, right):
    return lax.dot_general(left, right, ROWS_IN, preferred_element_type=F32)


def on_chip(value):
    return pltpu.with_memory_space_constraint(value, pltpu.VMEM)


def fill_tilde(tilde, amp, sums, pairs, across, e_left, e_right):
    width = tilde.shape[0]
    for left, right in pairs:
        amp[...] = gram(left[...], right[...])
        sums = [*sums, amp]
    for at in range(0, width, LANES):
        here = pl.ds(at, LANES)
        whole = sums[0][here, :]
        for other in sums[1:]:
            whole = whole + other[here, :]
        down = jnp.transpose(jnp.broadcast_to(across[:, at : at + LANES], (LANES, LANES)))
        amp[here, :] = whole / (down[:, :1] + across - e_left - e_right)
    for at in range(0, width, LANES):
        here = pl.ds(at, LANES)
        tilde[here, :] = (2.0 * amp[here, :] - jnp.transpose(amp[:, at : at + LANES])).astype(BF16)


def gram_kernel(block, offset, has_start, *refs):
    start, left, right, out = refs if has_start else (None, *refs)
    out[...] = start[...] if has_start else jnp.zeros_like(out)

    @pl.loop(0, left.shape[0] // block)
    def _(step):
        rows = left[pl.ds(pl.multiple_of(step * block, block), block), :]
        others = right[pl.ds(pl.multiple_of(offset + step * block, math.gcd(offset, block)), block), :]
        out[...] += gram(rows, others)


def gram_stage(left, right, offset=0, start=None):
    width = right.shape[1]
    vmem = pl.BlockSpec(memory_space=pltpu.VMEM)
    operands = [value for value in (start, left, right) if value is not None]
    return pl.pallas_call(
        functools.partial(gram_kernel, largest_block(left.shape[0], 640), offset, start is not None),
        in_specs=[vmem] * len(operands),
        out_specs=vmem,
        out_shape=pltpu.VMEM((width, width), F32),
        compiler_params=pltpu.CompilerParams(vmem_limit_bytes=4 << 20),
        cost_estimate=pl.CostEstimate(flops=2 * left.size * width, bytes_accessed=0, transcendentals=0),
        name="gram_stage",
    )(*[on_chip(value) for value in operands])


def near_kernel(n_sums, heights, energy, virt_row, *refs):
    sums, refs = refs[: 2 * n_sums], refs[2 * n_sums :]
    behind, ahead = refs[: len(heights)], refs[len(heights) : 2 * len(heights)]
    out, amp, *tildes = refs[2 * len(heights) :]
    across = virt_row[...]
    for item, tilde in enumerate(tildes):
        terms = sums[item * n_sums : (item + 1) * n_sums]
        fill_tilde(tilde, amp, terms, [], across, energy[2 * item], energy[2 * item + 1])

    first = 0
    for height, left, right in zip(heights, behind, ahead):
        block = largest_block(height, 640)

        @pl.loop(0, height // block)
        def _(step, first=first, block=block, left=left, right=right):
            here = pl.ds(pl.multiple_of(step * block, block), block)
            there = pl.ds(pl.multiple_of(first + step * block, math.gcd(first, block)), block)
            term = jnp.dot(left[here, :], tildes[0][...], preferred_element_type=F32)
            out[there, :] = term + jnp.dot(right[here, :], tildes[1][...], preferred_element_type=F32)

        first += height


def near_stage(energy, virt_row, sums, behind, ahead):
    heights = tuple(part.shape[0] for part in behind)
    rows, width = sum(heights), behind[0].shape[1]
    vmem = pl.BlockSpec(memory_space=pltpu.VMEM)
    operands = [virt_row, *sums, *behind, *ahead]
    return pl.pallas_call(
        functools.partial(near_kernel, len(sums) // 2, heights),
        in_specs=[pl.BlockSpec(memory_space=pltpu.SMEM)] + [vmem] * len(operands),
        out_specs=vmem,
        out_shape=pltpu.VMEM((rows, width), F32),
        scratch_shapes=[pltpu.VMEM((width, width), F32)] + [pltpu.VMEM((width, width), BF16)] * 2,
        compiler_params=pltpu.CompilerParams(vmem_limit_bytes=NEAR_VMEM),
        cost_estimate=pl.CostEstimate(flops=4 * rows * width * width, bytes_accessed=0, transcendentals=0),
        name="near_stage",
    )(energy, *[on_chip(value) for value in operands])


def far_kernel(block, n_sums, n_pairs, heights, energy, virt_row, *refs):
    refs = list(refs)
    sums = [refs.pop(0) for _ in range(n_sums)]
    pairs = [(refs.pop(0), refs.pop(0)) for _ in range(n_pairs)]
    parts = [refs.pop(0) for _ in heights]
    base, out, amp, tilde, out_buf, out_sem = refs
    width = tilde.shape[0]
    strips = width // LANES
    fill_tilde(tilde, amp, sums, pairs, virt_row[...], energy[0], energy[1])

    jobs, first = [], 0
    for part, height in zip(parts, heights):
        for at in range(0, height, block):
            jobs.append((part, at, first + at, min(block, height - at)))
        first += height

    def copy(job):
        _, _, row, tall = jobs[job]
        rows = pl.ds(0, tall * strips)
        return pltpu.make_async_copy(
            out_buf.at[job % 2, rows, :], out.at[pl.ds(row * strips, tall * strips), :], out_sem.at[job % 2]
        )

    for job, (part, at, row, tall) in enumerate(jobs):
        term = jnp.dot(part[pl.ds(at, tall), :], tilde[...], preferred_element_type=F32)
        result = base[pl.ds(row, tall), :] + term
        if job >= 2:
            copy(job - 2).wait()
        for strip in range(strips):
            out_buf[job % 2, pl.ds(strip, tall, strips), :] = result[:, strip * LANES : (strip + 1) * LANES]
        copy(job).start()
    for job in range(max(0, len(jobs) - 2), len(jobs)):
        copy(job).wait()


def far_stage(energy, virt_row, sums, pairs, parts, base, block):
    rows, width = base.shape
    strips = width // LANES
    vmem = pl.BlockSpec(memory_space=pltpu.VMEM)
    operands = [virt_row, *sums, *[value for pair in pairs for value in pair], *parts, base]
    heights = tuple(part.shape[0] for part in parts)
    return pl.pallas_call(
        functools.partial(far_kernel, block, len(sums), len(pairs), heights),
        in_specs=[pl.BlockSpec(memory_space=pltpu.SMEM)] + [vmem] * len(operands),
        out_specs=pl.BlockSpec(memory_space=pl.ANY),
        out_shape=jax.ShapeDtypeStruct((rows * strips, LANES), F32),
        scratch_shapes=[
            pltpu.VMEM((width, width), F32),
            pltpu.VMEM((width, width), BF16),
            pltpu.VMEM((2, block * strips, LANES), F32),
            pltpu.SemaphoreType.DMA((2,)),
        ],
        compiler_params=pltpu.CompilerParams(vmem_limit_bytes=14 << 20),
        cost_estimate=pl.CostEstimate(
            flops=2 * rows * width * width, bytes_accessed=4 * rows * width, transcendentals=0
        ),
        name="far_stage",
    )(energy, *[on_chip(value) for value in operands])


def plain(factors, occ_energy, virt_energy):
    rows, count, width = factors.shape
    n_blocks = lax.axis_size("occ")
    offset = n_blocks // 4
    index = lax.axis_index("occ")
    total = jnp.zeros((rows, count, width), F32)
    own_e = lax.dynamic_slice_in_dim(occ_energy, index * count, count)
    for steps, first in ((-offset, True), (offset, False)):
        ring = [(source, (source + steps) % n_blocks) for source in range(n_blocks)]
        other = lax.ppermute(factors, "occ", ring)
        other_e = lax.dynamic_slice_in_dim(occ_energy, (index - steps) % n_blocks * count, count)
        whole = sum(aux_terms(jnp.einsum("pja,pib->jaib", other, factors, preferred_element_type=F32)))
        e_left, e_right = (own_e[None, None, :, None], other_e[:, None, None, None])
        if not first:
            e_left, e_right = e_right, e_left
        amplitude = whole / (virt_energy[None, :, None, None] + virt_energy - e_left - e_right)
        tilde = (2.0 * amplitude - amplitude.transpose(0, 3, 2, 1)).astype(BF16)
        total = total + jnp.einsum("pja,jaib->pib", other, tilde, preferred_element_type=F32)
    return total


def cuts_of(rows, shares):
    unit, rest = divmod(rows, sum(shares))
    if rest or unit % 16:
        return [0, rows]
    return [unit * sum(shares[:at]) for at in range(len(shares) + 1)]


def sent(pieces, ring):
    arrived = []
    for piece in pieces:
        arrived.append(lax.ppermute(piece, "occ", ring))
    return arrived


def grams_of(parts, own, cuts, start=None):
    for part, at in zip(parts, cuts):
        if start is not None:
            part, start = lax.optimization_barrier((part, start))
        start = gram_stage(part, own, at, start)
    return start


def local(factors, occ_energy, virt_energy):
    rows, count, width = factors.shape
    n_blocks = lax.axis_size("occ")
    if count != 1 or width % LANES or rows % 16:
        return plain(factors, occ_energy, virt_energy)
    offset = n_blocks // 4
    index = lax.axis_index("occ")
    near_cuts, far_cuts, n_late = [0, rows], [0, rows], 0
    if lax.axis_size("aux") == 2:
        near_cuts = cuts_of(rows, NEAR_SHARES)
        far_cuts = cuts_of(rows, FAR_SHARES)
        n_late = int(len(far_cuts) > 2)

    up = [(s, s + offset) for s in range(n_blocks - offset)]
    down = [(s + offset, s) for s in range(n_blocks - offset)]
    ends = [(s, s + n_blocks - offset) for s in range(offset)]
    ends = ends + [(t, s) for s, t in ends]

    own = factors.reshape(rows, width)
    pieces = [own[a:b] for a, b in zip(near_cuts[:-1], near_cuts[1:])]
    behind, ahead = sent(pieces, up), sent(pieces, down)

    pieces = [own[a:b] for a, b in zip(far_cuts[:-1], far_cuts[1:])]
    at = max(0, len(behind) - 2)
    pieces[0], behind[at], ahead[at] = lax.optimization_barrier((pieces[0], behind[at], ahead[at]))
    *pieces[1:], behind[-1], ahead[-1] = lax.optimization_barrier((*pieces[1:], behind[-1], ahead[-1]))
    far = sent(pieces, ends)

    e_own = occ_energy[index]
    e_ahead = occ_energy[(index + offset) % n_blocks]
    e_behind = occ_energy[(index - offset) % n_blocks]
    virt_row = virt_energy.reshape(1, width)

    last = index >= n_blocks - offset
    energy = jnp.stack([e_behind, e_own, e_own, e_ahead])
    far_energy = jnp.stack([jnp.where(last, e_own, e_behind), jnp.where(last, e_ahead, e_own)])
    others = [swapped(piece) for piece in pieces[len(pieces) - n_late :]]
    energy, far_energy, *others = lax.optimization_barrier((energy, far_energy, *others))
    grams = [grams_of(parts[:-1], own, near_cuts) for parts in (behind, ahead)]
    close = [grams_of(parts[-1:], own, near_cuts[-2:-1], start) for parts, start in zip((behind, ahead), grams)]
    grams = close
    sums = aux_terms(grams[0]) + aux_terms(grams[1])
    base = near_stage(energy, virt_row, sums, behind, ahead)

    far[0], base = lax.optimization_barrier((far[0], base))
    sums = aux_terms(grams_of(far[: len(far) - n_late], own, far_cuts))
    pairs = []
    if n_late:
        pairs = [(swapped(far[-1]), others[0])]
        sums[0] = gram_stage(far[-1], own, far_cuts[-2], sums[0])
    out = far_stage(far_energy, virt_row, sums, pairs, far, base, min(rows, 768))
    return out.reshape(rows, count, width)


def solution(mesh):
    in_specs = (P("aux", "occ", None), P(), P())
    out_specs = P("aux", "occ", None)

    return jax.shard_map(local, mesh=mesh, in_specs=in_specs, out_specs=out_specs, check_vma=False)
```
